32 devices in a mesh: dp: 16 (over z, y, core), mp: 2 (over x).
Axes of the slice: x: 2, y: 2, z: 4, core: 2. Of those that a mesh axis runs over, the one named last changes fastest.
Arguments:
- tokens: bfloat16 [16384, 768], P('dp'), may hold values from -6 to 6
- time_embed: float32 [16, 768], P('dp'), may hold values from -4 to 4
- targets: bfloat16 [16384, 768], P('dp'), may hold values from -6 to 6
- buckets: int32 [16], P('dp'), may hold values from 0 to 15
- norm1_gain: float32 [768], replicated, may hold values from 0.5 to 1.5
- norm1_bias: float32 [768], replicated, may hold values from -1 to 1
- qkv_weight: bfloat16 [768, 3, 768], P(None, None, 'mp'), may hold values from -0.3125 to 0.3125
- qv_bias: float32 [2, 768], P(None, 'mp'), may hold values from -3 to 3
- out_weight: bfloat16 [768, 768], P('mp'), may hold values from -0.875 to 0.875
- out_bias: float32 [768], replicated, may hold values from -2 to 2
- norm2_gain: float32 [768], replicated, may hold values from 0.5 to 1.5
- norm2_bias: float32 [768], replicated, may hold values from -1 to 1
- up_weight: bfloat16 [768, 3072], P(None, 'mp'), may hold values from -0.21875 to 0.21875
- up_bias: float32 [3072], P('mp'), may hold values from -3 to 3
- down_weight: bfloat16 [3072, 768], P('mp'), may hold values from -0.109375 to 0.109375
- down_bias: float32 [768], replicated, may hold values from -2 to 2
Outputs:
- block_out: float32 [16384, 768], P('dp')
- loss: float32 [], replicated
- grad_tokens: float32 [16384, 768], P('dp')
- grad_time: float32 [16, 768], P('dp')
- grad_norm1_gain: float32 [768], P('dp')
- grad_norm1_bias: float32 [768], P('dp')
- grad_qkv_weight: float32 [768, 3, 768], P('dp', None, 'mp')
- grad_qv_bias: float32 [2, 768], P(None, 'mp')
- grad_out_weight: float32 [768, 768], P('mp', 'dp')
- grad_out_bias: float32 [768], P('dp')
- grad_norm2_gain: float32 [768], P('dp')
- grad_norm2_bias: float32 [768], P('dp')
- grad_up_weight: float32 [768, 3072], P('dp', 'mp')
- grad_up_bias: float32 [3072], P('mp')
- grad_down_weight: float32 [3072, 768], P('mp', 'dp')
- grad_down_bias: float32 [768], P('dp')
The draws below stay inside these ranges and needn't reach their ends.
All inputs are finite; a program needn't handle non-finite values.
Results may differ from the reference program's by a relative error of at most 0.0075.
The reference program's roundings to bfloat16 on the way count: a program that leaves them out, or rounds other values in their place, can miss the bound.
Values sent between devices are 32-bit elements; how exact they have to be, the bound alone decides.
A program may use at most 192 MiB of HBM per device.

```python
import math
import jax
import jax.numpy as jnp
import numpy as np
from jax import lax

D = 768
HEADS = 12
HEAD_DIM = 64
FF = 3072
LENGTH = 1024
BUCKETS = 16
SEQS = 16
TOKENS = 16384


def plant(array, own_key, smallest, top_value):
    shape = array.shape
    index_at = [jax.random.randint(jax.random.fold_in(own_key, axis), (), 0, shape[axis]) for axis in range(len(shape))]
    array = array.at[tuple(index_at)].set(smallest)
    longest = shape.index(max(shape))
    index_at[longest] = (index_at[longest] + 1) % shape[longest]
    return array.at[tuple(index_at)].set(top_value)


def strengthened(drawn, own_key, source, target, parts, factor):
    owner, partner = [(jnp.arange(drawn.shape[position]) // (drawn.shape[position] // parts)).reshape([-1 if axis == position else 1 for axis in range(drawn.ndim)]) for position in (source, target)]
    chosen = jax.random.permutation(own_key, parts)[partner]
    strong = (owner == chosen) | (owner == (partner + parts // 2) % parts)
    return jnp.where(strong, factor * drawn, drawn)


def steps_of(own_key, dims, cuts, smallest, high):
    loudness, own = 1.0, jax.random.fold_in(own_key, 6)
    for dim, shards_of in cuts:
        heights = jnp.exp(jax.random.uniform(jax.random.fold_in(own, dim), (shards_of,), jnp.float32, smallest / len(cuts), high / len(cuts)))
        loudness = loudness * jnp.repeat(heights, dims[dim] // shards_of).reshape([-1 if axis == dim else 1 for axis in range(len(dims))])
    return loudness


def cumulative_ranks(amount, lean):
    loads = [(1 << 20) // math.isqrt(grade ** lean) + 1 for grade in range(1, amount + 1)]
    scale = 1 + sum(loads) // (1 << 30)
    return np.cumsum(np.array([max(1, weight // scale) for weight in loads]))


def ranked(stream_key, extent, amount, skew):
    listing = cumulative_ranks(amount, skew)
    lot = jax.random.randint(jax.random.fold_in(stream_key, 1), extent, 0, int(listing[amount - 1]))
    rank = jnp.searchsorted(jnp.asarray(listing, jnp.int32), lot, side="right")
    return jax.random.permutation(jax.random.fold_in(stream_key, 2), amount)[rank].astype(jnp.int32)


def bell_draw(own_key, extent, scale, limit, shards=(), kind=jnp.bfloat16):
    level = steps_of(own_key, extent, shards, -0.22, 0.18) if shards else 1.0
    result = jax.random.normal(own_key, extent, jnp.float32) * scale * level
    return jnp.minimum(jnp.maximum(result, -limit), limit).astype(kind)


def bell_draw_with(key, dims, width, limit, pieces, heavy, kind=jnp.bfloat16):
    array = width * jax.random.normal(key, dims, jnp.float32)
    if pieces:
        array = array * steps_of(key, dims, pieces, -0.22, 0.18)
    return jnp.clip(strengthened(array, jax.random.fold_in(key, 3), *heavy), -limit, limit).astype(kind)


def setup_inputs(seed: int = 0) -> dict:
    keys = jax.random.split(jax.random.key(seed), 17)
    return {
        "tokens": bell_draw_with(keys[0], (TOKENS, D), 1.0, 6.0, ((0, 16),), (0, 1, 16, 2.0)),
        "time_embed": bell_draw(keys[1], (SEQS, D), 0.5, 4.0, ((0, 16),), jnp.float32),
        "targets": bell_draw_with(keys[2], (TOKENS, D), 1.0, 6.0, ((0, 16),), (0, 1, 16, 2.0)),
        "buckets": plant(ranked(keys[3], (SEQS,), BUCKETS, 2), jax.random.fold_in(keys[3], 3), 0, BUCKETS - 1).astype(jnp.int32),
        "norm1_gain": jnp.clip(1.0 + 0.1 * jax.random.normal(keys[4], (D,), jnp.float32), 0.5, 1.5),
        "norm1_bias": bell_draw(keys[5], (D,), 0.2, 1.0, (), jnp.float32),
        "qkv_weight": bell_draw(keys[6], (D, 3, D), (D // 2) ** -0.5, 0.3125, ((2, 2),)),
        "qv_bias": bell_draw(keys[7], (2, D), 0.5, 3.0, ((1, 2),), jnp.float32),
        "out_weight": bell_draw(keys[8], (D, D), (D // 16) ** -0.5, 0.875, ((0, 2),)),
        "out_bias": bell_draw(keys[9], (D,), 0.3, 2.0, (), jnp.float32),
        "norm2_gain": jnp.clip(1.0 + 0.1 * jax.random.normal(keys[10], (D,), jnp.float32), 0.5, 1.5),
        "norm2_bias": bell_draw(keys[11], (D,), 0.2, 1.0, (), jnp.float32),
        "up_weight": bell_draw(keys[12], (D, FF), D ** -0.5, 0.21875, ((1, 2),)),
        "up_bias": bell_draw(keys[13], (FF,), 0.5, 3.0, ((0, 2),), jnp.float32),
        "down_weight": bell_draw(keys[14], (FF, D), FF ** -0.5, 0.109375, ((0, 2),)),
        "down_bias": bell_draw(keys[15], (D,), 0.3, 2.0, (), jnp.float32),
    }


EPSILON = 1e-05
HIGHEST = lax.Precision.HIGHEST

@jax.custom_vjp
def low(v):
    return lax.optimization_barrier(v.astype(jnp.bfloat16)).astype(jnp.float32)

@jax.custom_vjp
def low_back(v):
    return v

def low_keep(v):
    return (low(v), None)

def low_pass(kept, grad):
    return (grad,)

def back_keep(v):
    return (v, None)

def back_low(kept, grad):
    return (low(grad),)
low.defvjp(low_keep, low_pass)
low_back.defvjp(back_keep, back_low)

def layer_norm(stream, gain_vec, bias_vec):
    centre = lax.optimization_barrier(jnp.mean(stream, axis=-1, keepdims=True))
    centered = stream - centre
    spread = lax.optimization_barrier(jnp.mean(centered * centered, axis=-1, keepdims=True))
    return centered * lax.rsqrt(spread + EPSILON) * gain_vec + bias_vec

def attend_block(query_block, key_heads, value_heads):
    scores = low_back(jnp.einsum('qhd,khd->hqk', query_block, key_heads, precision=HIGHEST) * 0.125)
    highest = lax.optimization_barrier(jnp.max(scores, axis=-1, keepdims=True))
    expo_terms = jnp.exp(scores - highest)
    attn_probs = low(expo_terms / lax.optimization_barrier(jnp.sum(expo_terms, axis=-1, keepdims=True)))
    return jnp.einsum('hqk,khd->qhd', attn_probs, value_heads, precision=HIGHEST)

def attend_sequence(query_heads, key_heads, value_heads):
    block_rows = min(512, LENGTH)
    query_blocks = query_heads.reshape(LENGTH // block_rows, block_rows, HEADS, HEAD_DIM)

    def one_block(query_block):
        return attend_block(query_block, key_heads, value_heads)
    mixed_heads = lax.map(jax.checkpoint(one_block), query_blocks)
    return mixed_heads.reshape(LENGTH, D)

def sequence_layer(params, seq_tokens, seq_time):
    gain_one, bias_one, qkv_full, qv_full, outw_full, outb_full, gain_two, bias_two, upw_full, upb_full, downw_full, downb_full = params
    stream_in = seq_tokens + seq_time[None, :]
    normed_in = low(layer_norm(stream_in, gain_one, bias_one))
    zero_row = jnp.zeros_like(qv_full[0])
    projected = jnp.dot(normed_in, qkv_full.reshape(D, 3 * D), precision=HIGHEST)
    projected = projected + jnp.concatenate([qv_full[0], zero_row, qv_full[1]])
    projected = low_back(low(projected))
    query_heads = projected[:, :D].reshape(LENGTH, HEADS, HEAD_DIM)
    key_heads = projected[:, D:2 * D].reshape(LENGTH, HEADS, HEAD_DIM)
    value_heads = projected[:, 2 * D:].reshape(LENGTH, HEADS, HEAD_DIM)
    attended = low_back(low(attend_sequence(query_heads, key_heads, value_heads)))
    attn_branch = low_back(jnp.dot(attended, outw_full, precision=HIGHEST) + outb_full)
    stream_mid = stream_in + attn_branch
    normed_mid = low(layer_norm(stream_mid, gain_two, bias_two))
    pre_act = low_back(jnp.dot(normed_mid, upw_full, precision=HIGHEST) + upb_full)
    hidden = low(jax.nn.gelu(pre_act, approximate=False))
    mlp_branch = low_back(jnp.dot(hidden, downw_full, precision=HIGHEST) + downb_full)
    return stream_mid + mlp_branch

def reference(tokens, time_embed, targets, buckets, norm1_gain, norm1_bias, qkv_weight, qv_bias, out_weight, out_bias, norm2_gain, norm2_bias, up_weight, up_bias, down_weight, down_bias):
    selector = (buckets[:, None] == jnp.arange(BUCKETS, dtype=jnp.int32)[None, :]).astype(jnp.float32)
    counts = lax.optimization_barrier(jnp.sum(selector, axis=0))
    count_floor = jnp.maximum(counts, 1.0)
    seq_weight = lax.optimization_barrier(jnp.sum(selector / count_floor[None, :], axis=1)) * (SEQS / (2.0 * BUCKETS))
    params = tuple((member.astype(jnp.float32) for member in (norm1_gain, norm1_bias, qkv_weight, qv_bias, out_weight, out_bias, norm2_gain, norm2_bias, up_weight, up_bias, down_weight, down_bias)))
    target_rows = targets.astype(jnp.float32).reshape(SEQS, LENGTH, D)

    def objective_fn(params, token_rows, time_rows):

        def step(running, member):
            seq_tokens, seq_time, seq_target, seq_scale = member
            seq_out = sequence_layer(params, seq_tokens, seq_time)
            misfit = seq_out - seq_target
            return (running + seq_scale * jnp.sum(misfit * misfit), seq_out)
        running, outputs = lax.scan(jax.checkpoint(step), jnp.zeros((), jnp.float32), (token_rows.reshape(SEQS, LENGTH, D), time_rows, target_rows, seq_weight))
        return (running, outputs)
    objective, pullback, outputs = jax.vjp(objective_fn, params, tokens.astype(jnp.float32), time_embed, has_aux=True)
    grad_params, grad_tokens, grad_time = pullback(jnp.ones((), jnp.float32))
    loss = objective * (2.0 / (SEQS * LENGTH * D))
    return (outputs.reshape(TOKENS, D), loss, grad_tokens, grad_time, grad_params[0], grad_params[1], grad_params[2], grad_params[3], grad_params[4], grad_params[5], grad_params[6], grad_params[7], grad_params[8], grad_params[9], grad_params[10], grad_params[11])
```

```python
import jax
import jax.numpy as jnp
from jax import lax
from jax.experimental import pallas as pl
from jax.experimental.pallas import tpu as pltpu
from jax.sharding import PartitionSpec as P

HEAD_DIM = 64
BUCKETS = 16
EPSILON = 1e-05
AXES = ("dp", "mp")


def layer_norm(stream, gain_vec, bias_vec):
    centre = jnp.mean(stream, axis=-1, keepdims=True)
    centered = stream - centre
    spread = jnp.mean(centered * centered, axis=-1, keepdims=True)
    inverse = lax.rsqrt(spread + EPSILON)
    normed = centered * inverse
    return (normed * gain_vec + bias_vec, normed, inverse)


def norm_back(upstream, normed, inverse, gain_vec):
    scaled = upstream * gain_vec
    first_mean = jnp.mean(scaled, axis=-1, keepdims=True)
    second_mean = jnp.mean(scaled * normed, axis=-1, keepdims=True)
    return inverse * (scaled - first_mean - normed * second_mean)


def gelu_slope(inputs):
    cumulative = 0.5 * (1.0 + lax.erf(inputs * 0.7071067811865476))
    density = jnp.exp(-0.5 * inputs * inputs) * 0.3989422804014327
    return cumulative + inputs * density


def over_rows(left_side, right_side):
    return lax.dot_general(
        left_side, right_side, (((0,), (0,)), ((), ())), preferred_element_type=jnp.float32
    )


def against(left_side, right_side):
    return lax.dot_general(
        left_side, right_side, (((1,), (1,)), ((), ())), preferred_element_type=jnp.float32
    )


def block_scores(query_block, key_heads):
    return (
        jnp.einsum("qhd,khd->hqk", query_block, key_heads, preferred_element_type=jnp.float32)
        * 0.125
    )


def attend_block(query_block, key_heads, value_heads):
    scores = block_scores(query_block, key_heads)
    highest = jnp.max(scores, axis=-1, keepdims=True)
    logsum = highest + jnp.log(jnp.sum(jnp.exp(scores - highest), axis=-1, keepdims=True))
    attn_probs = jnp.exp(scores - logsum).astype(jnp.bfloat16)
    mixed_heads = jnp.einsum(
        "hqk,khd->qhd", attn_probs, value_heads, preferred_element_type=jnp.float32
    )
    return (mixed_heads.astype(jnp.bfloat16), logsum[..., 0])


def attend_back(query_block, logsum, upstream, key_heads, value_heads):
    scores = block_scores(query_block, key_heads)
    exact_probs = jnp.exp(scores - logsum[..., None])
    grad_value = jnp.einsum(
        "hqk,qhd->khd",
        exact_probs.astype(jnp.bfloat16),
        upstream,
        preferred_element_type=jnp.float32,
    )
    grad_probs = jnp.einsum(
        "qhd,khd->hqk", upstream, value_heads, preferred_element_type=jnp.float32
    )
    centre = jnp.sum(grad_probs * exact_probs, axis=-1, keepdims=True)
    grad_scores = (exact_probs * (grad_probs - centre)).astype(jnp.bfloat16)
    grad_query = (
        jnp.einsum("hqk,khd->qhd", grad_scores, key_heads, preferred_element_type=jnp.float32)
        * 0.125
    )
    grad_key = (
        jnp.einsum("hqk,qhd->khd", grad_scores, query_block, preferred_element_type=jnp.float32)
        * 0.125
    )
    return (grad_query, grad_key, grad_value)


def attention(projected, local_width):
    length = projected.shape[0]
    heads = local_width // HEAD_DIM
    rows = min(512, length)
    queries = projected[:, :local_width].reshape(length // rows, rows, heads, HEAD_DIM)
    keys = projected[:, local_width : 2 * local_width].reshape(length, heads, HEAD_DIM)
    values = projected[:, 2 * local_width :].reshape(length, heads, HEAD_DIM)
    attended, logsum = lax.map(lambda block: attend_block(block, keys, values), queries)
    return attended.reshape(length, local_width), logsum


def attention_back(projected, logsum, upstream, local_width):
    length = projected.shape[0]
    heads = local_width // HEAD_DIM
    rows = min(512, length)
    queries = projected[:, :local_width].reshape(length // rows, rows, heads, HEAD_DIM)
    keys = projected[:, local_width : 2 * local_width].reshape(length, heads, HEAD_DIM)
    values = projected[:, 2 * local_width :].reshape(length, heads, HEAD_DIM)
    upstream = upstream.reshape(length // rows, rows, heads, HEAD_DIM)
    grad_query, grad_key, grad_value = lax.map(
        lambda member: attend_back(member[0], member[1], member[2], keys, values),
        (queries, logsum, upstream),
    )
    return jnp.concatenate(
        [
            grad_query.reshape(length, local_width),
            jnp.sum(grad_key, axis=0).reshape(length, local_width),
            jnp.sum(grad_value, axis=0).reshape(length, local_width),
        ],
        axis=1,
    ).astype(jnp.bfloat16)


def assemble_kernel(flags, own_ref, first_ref, second_ref, whole_ref):
    at_home = flags[0] == 1
    from_first = (pl.program_id(0) * 2 // pl.num_programs(0)) == flags[1]

    @pl.when(at_home)
    def _():
        whole_ref[...] = own_ref[...]

    @pl.when(jnp.logical_not(at_home) & from_first)
    def _():
        whole_ref[...] = first_ref[...].astype(jnp.bfloat16)

    @pl.when(jnp.logical_not(at_home) & jnp.logical_not(from_first))
    def _():
        whole_ref[...] = second_ref[...].astype(jnp.bfloat16)


def assemble(own, first, second, flags):
    rows, width = own.shape
    per_half = 2
    block = rows // (2 * per_half)

    def own_map(i, flags):
        return (jnp.where(flags[0] == 1, i, 0), 0)

    def part_map(half, i, flags):
        step = jnp.clip(i - half * per_half, 0, per_half - 1)
        return (jnp.where(flags[0] == 1, 0, step), 0)

    def first_map(i, flags):
        return part_map(flags[1], i, flags)

    def second_map(i, flags):
        return part_map(1 - flags[1], i, flags)

    return pl.pallas_call(
        assemble_kernel,
        grid_spec=pltpu.PrefetchScalarGridSpec(
            num_scalar_prefetch=1,
            grid=(2 * per_half,),
            in_specs=[
                pl.BlockSpec((block, width), own_map),
                pl.BlockSpec((block, width), first_map),
                pl.BlockSpec((block, width), second_map),
            ],
            out_specs=pl.BlockSpec((block, width), lambda i, flags: (i, 0)),
        ),
        out_shape=jax.ShapeDtypeStruct((rows, width), jnp.bfloat16),
        cost_estimate=pl.CostEstimate(flops=0, bytes_accessed=rows * width * 8, transcendentals=0),
        name="assemble",
    )(flags, own, first, second)


class Routes:
    def __init__(self, mesh):
        self.groups = mesh.shape["dp"] // 2

    def perm(self, target):
        found = []
        for g in range(self.groups):
            for c in range(2):
                for x in range(2):
                    where = target(g, c, x)
                    if where is not None:
                        tg, tc, tx = where
                        found.append(((g * 2 + c) * 2 + x, (tg * 2 + tc) * 2 + tx))
        return found

    def move(self, value, target):
        return lax.ppermute(value, AXES, self.perm(target))

    def swap_cores(self, value):
        return self.move(value, lambda g, c, x: (g, 1 - c, x))

    def home_to_core(self, value):
        return self.move(value, lambda g, c, x: (g, 1 - c, x) if c == x else None)

    def home_to_side(self, value):
        return self.move(value, lambda g, c, x: (g, c, 1 - x) if c == x else None)

    def away_pairs(self, value):
        return self.move(value, lambda g, c, x: (g ^ 1, c, x) if c != x else None)

    def flip_group(self, value, bit):
        return self.move(value, lambda g, c, x: (g ^ bit, c, x))

    def flip_side(self, value):
        return self.move(value, lambda g, c, x: (g, c, 1 - x))

    def sum_groups(self, value):
        bit = 1
        while bit < self.groups:
            value = value + self.flip_group(value, bit)
            bit *= 2
        return value

    def sum_sequences(self, value):
        return self.flip_side(self.sum_groups(value)) + self.sum_groups(value)


def solution(mesh):
    routes = Routes(mesh)
    dp = mesh.shape["dp"]

    def shards(
        tokens,
        time_embed,
        targets,
        buckets,
        norm1_gain,
        norm1_bias,
        qkv_weight,
        qv_bias,
        out_weight,
        out_bias,
        norm2_gain,
        norm2_bias,
        up_weight,
        up_bias,
        down_weight,
        down_bias,
    ):
        f32 = jnp.float32
        length, model_width = tokens.shape
        local_width = qkv_weight.shape[2]
        d = lax.axis_index("dp")
        side = lax.axis_index("mp")
        core = d % 2
        group = d // 2
        low = group % 2
        home = core == side
        flags = jnp.stack([home.astype(jnp.int32), low.astype(jnp.int32)])

        def pick(own, received):
            return jnp.where(home, own, received)

        def fetch(weight):
            rows = weight.shape[0] // 2
            part = lax.dynamic_slice_in_dim(weight, low * rows, rows, 0).astype(f32)
            first = routes.home_to_side(part)
            second = routes.away_pairs(first)
            return assemble(weight, first, second, flags)

        selector = (buckets[:, None] == jnp.arange(BUCKETS, dtype=jnp.int32)[None, :]).astype(f32)
        own_counts = jnp.sum(selector, axis=0)
        counts = routes.sum_groups(own_counts + routes.swap_cores(own_counts))
        my_selector = pick(own_counts, routes.home_to_core(own_counts))
        count_floor = jnp.maximum(counts, 1.0)
        weight_of = jnp.sum(my_selector / count_floor)
        seq_weight = weight_of * (dp / BUCKETS)

        flat_bias = jnp.concatenate([qv_bias, up_bias.reshape(-1, qv_bias.shape[1])], axis=0)
        flat_bias = pick(flat_bias, routes.home_to_side(flat_bias))
        qv_bias = flat_bias[:2]
        up_bias = flat_bias[2:].reshape(-1)

        flat_qkv = fetch(qkv_weight.reshape(model_width, 3 * local_width))
        own_stream = tokens.astype(f32) + time_embed
        stream_in = pick(own_stream, routes.home_to_core(own_stream))
        own_targets = targets.astype(f32)
        goal = pick(own_targets, routes.home_to_core(own_targets))
        out_weight = fetch(out_weight)
        up_weight = fetch(up_weight)
        down_weight = fetch(down_weight)

        normed_in, unit_one, inverse_one = layer_norm(stream_in, norm1_gain, norm1_bias)
        normed_in = normed_in.astype(jnp.bfloat16)
        full_bias = jnp.concatenate([qv_bias[0], jnp.zeros_like(qv_bias[0]), qv_bias[1]])
        projected = (
            jnp.dot(normed_in, flat_qkv, preferred_element_type=f32) + full_bias
        ).astype(jnp.bfloat16)
        attended, logsum = attention(projected, local_width)
        attn_part = jnp.dot(attended, out_weight, preferred_element_type=f32)
        attn_sum = attn_part + routes.swap_cores(attn_part)
        stream_mid = stream_in + (attn_sum + out_bias)
        normed_mid, unit_two, inverse_two = layer_norm(stream_mid, norm2_gain, norm2_bias)
        normed_mid = normed_mid.astype(jnp.bfloat16)
        pre_act = jnp.dot(normed_mid, up_weight, preferred_element_type=f32) + up_bias
        hidden = jax.nn.gelu(pre_act, approximate=False).astype(jnp.bfloat16)
        down_part = jnp.dot(hidden, down_weight, preferred_element_type=f32)
        down_sum = down_part + routes.swap_cores(down_part)
        block_out = stream_mid + (down_sum + down_bias)
        misfit = block_out - goal
        seq_loss = jnp.sum(misfit * misfit) * weight_of
        grad_out = misfit * seq_weight
        grad_mixed = grad_out.astype(jnp.bfloat16)
        block_result = pick(block_out, routes.home_to_side(block_out))

        def rows_to_blocks(grad):
            return grad.reshape(routes.groups // 2, 2, 2, model_width // dp, grad.shape[1])

        def take(value, index, axis):
            return lax.dynamic_index_in_dim(value, index, axis, keepdims=False)

        def over_low(value):
            return take(value, low, 1) + routes.flip_group(take(value, 1 - low, 1), 1)

        def over_side(value, axis):
            zero = jnp.take(value, 0, axis=axis)
            one = jnp.take(value, 1, axis=axis)
            to_zero = routes.move(zero, lambda g, c, x: (g, 0, c) if x != c else None)
            to_one = routes.move(one, lambda g, c, x: (g, 1, c) if x != c else None)
            across = routes.home_to_core(take(value, 1 - core, axis))
            arrived = jnp.where(core == 0, to_zero, to_one)
            return arrived + pick(take(value, core, axis), across)

        def over_high(value):
            bits = routes.groups // 2
            high = group // 2
            bit = 1
            while value.shape[0] > 1:
                half = value.reshape((value.shape[0] // 2, 2) + value.shape[1:])
                mine = (high // bit) % 2
                value = take(half, mine, 1) + routes.flip_group(take(half, 1 - mine, 1), 2 * bit)
                bit *= 2
            assert bit == bits
            return value[0]

        def scatter(grad, low_first):
            blocks = rows_to_blocks(grad)
            if low_first:
                blocks = over_side(over_low(blocks), 1)
            else:
                blocks = over_low(over_side(blocks, 2))
            return over_high(blocks)

        grad_down_bias = jnp.sum(grad_mixed, axis=0, dtype=f32)
        grad_down_weight = scatter(over_rows(grad_mixed, hidden), False)
        grad_hidden = against(grad_mixed, down_weight)
        grad_pre = (grad_hidden * gelu_slope(pre_act)).astype(jnp.bfloat16)
        grad_up_bias = jnp.sum(grad_pre, axis=0, dtype=f32)
        mid_part = against(grad_pre, up_weight)
        grad_normed_mid = mid_part + routes.swap_cores(mid_part)
        grad_up_weight = scatter(over_rows(normed_mid, grad_pre), True)
        grad_gain_two = jnp.sum(grad_normed_mid * unit_two, axis=0)
        grad_bias_two = jnp.sum(grad_normed_mid, axis=0)
        grad_mid = grad_out + norm_back(grad_normed_mid, unit_two, inverse_two, norm2_gain)
        grad_attn = grad_mid.astype(jnp.bfloat16)
        grad_out_bias = jnp.sum(grad_attn, axis=0, dtype=f32)
        grad_out_weight = scatter(over_rows(grad_attn, attended), True)
        grad_attended = against(grad_attn, out_weight).astype(jnp.bfloat16)
        grad_proj = attention_back(projected, logsum, grad_attended, local_width)
        in_part = against(grad_proj, flat_qkv)
        grad_normed_in = in_part + routes.swap_cores(in_part)
        grad_qkv_weight = scatter(over_rows(normed_in, grad_proj), True)
        proj_sums = jnp.sum(grad_proj, axis=0, dtype=f32)
        grad_gain_one = jnp.sum(grad_normed_in * unit_one, axis=0)
        grad_bias_one = jnp.sum(grad_normed_in, axis=0)
        grad_tokens = grad_mid + norm_back(grad_normed_in, unit_one, inverse_one, norm1_gain)
        tokens_result = pick(grad_tokens, routes.home_to_side(grad_tokens))
        grad_time = jnp.sum(tokens_result, axis=0, keepdims=True)

        early = jnp.concatenate(
            [grad_down_bias, grad_up_bias, jnp.full((128,), seq_loss), grad_gain_two, grad_bias_two, grad_out_bias]
        )
        late = jnp.concatenate([proj_sums, grad_gain_one, grad_bias_one])
        early = routes.sum_sequences(early)
        late = routes.sum_sequences(late)
        hidden_width = up_bias.shape[0]
        halves = jnp.concatenate(
            [early[model_width : model_width + hidden_width], late[: 3 * local_width]]
        )
        halves = pick(halves, routes.swap_cores(halves))
        grad_up_bias = halves[:hidden_width]
        proj_sums = halves[hidden_width:].reshape(3, local_width)
        grad_qv_bias = jnp.stack([proj_sums[0], proj_sums[2]])
        after = model_width + hidden_width
        loss = early[after] / BUCKETS / (length * model_width)
        share = model_width // dp

        def mine(vector):
            return lax.dynamic_slice_in_dim(vector, d * share, share, 0)

        after += 128
        grad_down_bias = mine(early[:model_width])
        grad_gain_two = mine(early[after : after + model_width])
        grad_bias_two = mine(early[after + model_width : after + 2 * model_width])
        grad_out_bias = mine(early[after + 2 * model_width :])
        grad_gain_one = mine(late[3 * local_width : 3 * local_width + model_width])
        grad_bias_one = mine(late[3 * local_width + model_width :])
        return (
            block_result,
            loss,
            tokens_result,
            grad_time,
            grad_gain_one,
            grad_bias_one,
            grad_qkv_weight.reshape(share, 3, local_width),
            grad_qv_bias,
            grad_out_weight.T,
            grad_out_bias,
            grad_gain_two,
            grad_bias_two,
            grad_up_weight,
            grad_up_bias,
            grad_down_weight.T,
            grad_down_bias,
        )

    return jax.shard_map(
        shards,
        mesh=mesh,
        in_specs=(
            P("dp", None),
            P("dp", None),
            P("dp", None),
            P("dp"),
            P(),
            P(),
            P(None, None, "mp"),
            P(None, "mp"),
            P("mp", None),
            P(),
            P(),
            P(),
            P(None, "mp"),
            P("mp"),
            P("mp", None),
            P(),
        ),
        out_specs=(
            P("dp", None),
            P(),
            P("dp", None),
            P("dp", None),
            P("dp"),
            P("dp"),
            P("dp", None, "mp"),
            P(None, "mp"),
            P("mp", "dp"),
            P("dp"),
            P("dp"),
            P("dp"),
            P("dp", "mp"),
            P("mp"),
            P("mp", "dp"),
            P("dp"),
        ),
        check_vma=False,
    )
```
